256 devices in a mesh: dp: 64 (over z, x, core), tensor: 4 (over y).
Axes of the slice: x: 4, y: 4, z: 8, core: 2. Of those that a mesh axis runs over, the one named last changes fastest.
Arguments:
- master_old: float32 [3072, 36864], P('dp', 'tensor'), may hold values from -6 to 6
- moment1_old: float32 [3072, 36864], P('dp', 'tensor'), may hold values from -4 to 4
- moment2_old: float32 [3072, 36864], P('dp', 'tensor'), may hold values from 0.0001 to 1
- grad: bfloat16 [3072, 36864], P('dp', 'tensor'), may hold values from -28 to 28
- send_slots: int32 [64, 1728], P('dp'), may hold values from 0 to 1727, each once within a row
- recv_slots: int32 [64, 1728], P('dp'), may hold values from 0 to 1727, each once within a row
Outputs:
- master_new: float32 [3072, 36864], P('dp', 'tensor')
- moment1_new: float32 [3072, 36864], P('dp', 'tensor')
- moment2_new: float32 [3072, 36864], P('dp', 'tensor')
The draws below stay inside these ranges and needn't reach their ends.
Inputs may be any that keep to these rules, and one draw needn't show every extreme that they name: `send_slots`: each row is a permutation of 0 to 1727; entry [i, j * 27 + q] is the old slot of the q-th block that device i of dp sends to device j. `recv_slots`: each row is a permutation of 0 to 1727; entry [j, i * 27 + q] is the new slot on device j of the q-th block from device i.
All inputs are finite; a program needn't handle non-finite values.
Results may differ from the reference program's by a relative error of at most 0.0003.
Values sent between devices are 32-bit elements; how exact they have to be, the bound alone decides.
A program may use at most 64 MiB of HBM per device.

```python
import math
import jax
import jax.numpy as jnp

ROWS = 3072
FF = 36864
SEGW = 128
RD = 48
COLS = 9216
HALF = 4608
NSEG = 36
BLK_DEV = 1728
PER_PEER = 27
N_DP = 64
N_TENSOR = 4


def draw_grad(key, part):
    base_key = jax.random.fold_in(key, 11)
    key_base, key_column = jax.random.split(base_key, 2)
    position = jnp.arange(ROWS, dtype=jnp.float32) / (ROWS - 1)
    column_log = jax.random.uniform(key_column, (FF,), jnp.float32, -1.15, 1.15)
    column_scale = jnp.exp(column_log) / 1.465
    row_scale = jnp.power(10.0, position - 0.5) / 1.4664
    values = jax.random.truncated_normal(key_base, -6.0, 6.0, (ROWS, FF), jnp.float32)
    return (values * row_scale[:, None] * column_scale[None, :]).astype(jnp.bfloat16)


def steps_of(stream_key, shape, cuts, low, largest):
    factor_of = 1.0
    for axis_at, blocks in cuts:
        draws = jax.random.uniform(jax.random.fold_in(jax.random.fold_in(stream_key, 6), axis_at), (blocks,), jnp.float32, low / len(cuts), largest / len(cuts))
        factor_of = factor_of * jnp.repeat(jnp.exp(draws), shape[axis_at] // blocks).reshape((-1,) + (1,) * (len(shape) - 1 - axis_at))
    return factor_of


def bell_draw(rng, dims, width, most, shards=(), kind=jnp.bfloat16):
    array = width * jax.random.normal(rng, dims, jnp.float32)
    if shards:
        array = array * steps_of(rng, dims, shards, -0.22, 0.18)
    return jnp.clip(array, -most, most).astype(kind)


def setup_inputs(seed: int = 0) -> dict:
    streams_of = jax.random.split(jax.random.key(seed), 7)
    return {
        "master_old": bell_draw(streams_of[0], (ROWS, FF), 1.0, 6.0, ((0, 64), (1, 4)), jnp.float32),
        "moment1_old": bell_draw(streams_of[1], (ROWS, FF), 0.3, 4.0, ((0, 64), (1, 4)), jnp.float32),
        "moment2_old": jnp.clip(jnp.exp(math.log(1.0) - 9.2103404 * jax.random.uniform(streams_of[2], (ROWS, FF), jnp.float32) ** steps_of(streams_of[2], (ROWS, FF), ((0, 64), (1, 4)), -0.2, 0.2)), 0.0001, 1.0),
        "grad": draw_grad(jax.random.fold_in(streams_of[6], 71), 0),
        "send_slots": jax.vmap(lambda own: jax.random.permutation(own, BLK_DEV))(jax.random.split(streams_of[4], N_DP)).reshape((N_DP, BLK_DEV)).astype(jnp.int32),
        "recv_slots": jax.vmap(lambda own: jax.random.permutation(own, BLK_DEV))(jax.random.split(streams_of[5], N_DP)).reshape((N_DP, BLK_DEV)).astype(jnp.int32),
    }


beta_one = 0.9
beta_two = 0.95
correct_one = 0.6513215599
correct_two = 0.4012630608
adam_eps = 1e-08
learning_rate = 0.01
weight_decay = 0.1
clip_ratio = 0.75

def move_shard(shard, send_slots, recv_slots):
    tiles = shard.reshape(N_DP, RD, 2, NSEG, SEGW).transpose(0, 1, 3, 2, 4).reshape(N_DP, BLK_DEV, 2, SEGW)
    outgoing = jnp.take_along_axis(tiles, send_slots[:, :, None, None], axis=1)
    arrived = outgoing.reshape(N_DP, N_DP, PER_PEER, 2, SEGW).transpose(1, 0, 2, 3, 4).reshape(N_DP, BLK_DEV, 2, SEGW)
    sources = jnp.arange(N_DP, dtype=jnp.int32)[:, None]
    placed = jnp.zeros_like(arrived).at[sources, recv_slots].set(arrived)
    return placed.reshape(N_DP, RD, NSEG, 2, SEGW).transpose(0, 1, 3, 2, 4).reshape(ROWS, COLS)

def reshard(matrix, send_slots, recv_slots):
    moved = [move_shard(matrix[:, shard_index * COLS:(shard_index + 1) * COLS], send_slots, recv_slots) for shard_index in range(N_TENSOR)]
    pieces = []
    for pair_index in range(N_TENSOR // 2):
        first = moved[2 * pair_index]
        second = moved[2 * pair_index + 1]
        pieces.append(first[:, :HALF])
        pieces.append(second[:, :HALF])
        pieces.append(first[:, HALF:])
        pieces.append(second[:, HALF:])
    return jnp.concatenate(pieces, axis=1)

def reference(master_old, moment1_old, moment2_old, grad, send_slots, recv_slots):
    new_master = reshard(master_old, send_slots, recv_slots)
    new_first = reshard(moment1_old, send_slots, recv_slots)
    new_second = reshard(moment2_old, send_slots, recv_slots)
    wide = grad.astype(jnp.float32)
    sum_squares = jnp.sum(wide * wide)
    limit = clip_ratio * jnp.sqrt(jnp.float32(ROWS * FF))
    clip_scale = jnp.minimum(1.0, limit / jnp.sqrt(sum_squares + 1e-06))
    scaled = clip_scale * wide
    moment1 = beta_one * new_first + (1.0 - beta_one) * scaled
    moment2 = beta_two * new_second + (1.0 - beta_two) * scaled * scaled
    update = moment1 / correct_one / (jnp.sqrt(moment2 / correct_two) + adam_eps)
    master = new_master - learning_rate * (update + weight_decay * new_master)
    return (master, moment1, moment2)
```

```python
import functools

import jax
import jax.numpy as jnp
from jax import lax
from jax.experimental import pallas as pl
from jax.experimental.pallas import tpu as pltpu
from jax.sharding import PartitionSpec as P

ROWS = 3072
FF = 36864
SEGW = 128
RD = 48
COLS = 9216
HALF = 4608
NSEG = 36
BLOCKS = 1728
N_DP = 64
PER_PEER = 27
TILES = 2 * BLOCKS
MESH = pl.DeviceIdType.MESH

beta_one = 0.9
beta_two = 0.95
correct_one = 0.6513215599
correct_two = 0.4012630608
adam_eps = 1e-08
learning_rate = 0.01
weight_decay = 0.1
clip_ratio = 0.75

CHUNK = 512


def kernel(
    send_ref, place_ref, first_hbm, second_hbm, master_hbm, grad_hbm,
    first_out, second_out, master_out,
    old0, old1, old2, send0, send1, send2, recv0, recv1, recv2, new0, new1, new2,
    grad, update, pair_rows, own_row, all_rows, inverse, inverse_smem,
    load_sems, out_sems, send_sem, recv_sems, small_send, small_recv, table_sem,
):
    me = lax.axis_index("dp")
    shard = lax.axis_index("tensor")
    z, x, core = me // 8, (me // 2) % 4, me % 2
    parity = shard % 2
    even_shard = shard - parity
    olds, sends, recvs, news = (old0, old1, old2), (send0, send1, send2), (recv0, recv1, recv2), (new0, new1, new2)
    outs = (first_out, second_out, master_out)

    def peer_of(n):
        zi, xi = n % 8, (n // 8) % 4
        other_shard, other_core = 1 - (n // 32) % 2, 1 - n // 64
        dz = jnp.where(zi % 2 == 0, 4 + zi // 2, 3 - zi // 2)
        jz = (z + dz) % 8
        jx = (x + xi + 1) % 4
        jc = (core + other_core) % 2
        half = (parity + other_shard) % 2
        return (jz * 4 + jx) * 2 + jc, half

    barrier = pltpu.get_barrier_semaphore()

    @pl.loop(0, 127)
    def _(n):
        j, half = peer_of(n)
        pl.semaphore_signal(barrier, inc=1, device_id=(j, even_shard + half), device_id_type=MESH)

    far_shards = [(shard + k) % 4 for k in (1, 2, 3)]
    for k in (1, 2, 3):
        pl.semaphore_signal(barrier, inc=1, device_id=(me, (shard + k) % 4), device_id_type=MESH)

    loads = [
        pltpu.make_async_copy(source, target, load_sems.at[k])
        for k, (source, target) in enumerate(
            [(grad_hbm, grad), (first_hbm, old0), (second_hbm, old1), (master_hbm, old2)]
        )
    ]
    for load in loads:
        load.start()

    loads[0].wait()

    def square(n, total):
        block = grad[n // 18, :, pl.ds(pl.multiple_of((n % 18) * CHUNK, CHUNK), CHUNK)].astype(jnp.float32)
        return total + block * block

    squares = lax.fori_loop(0, 54, square, jnp.zeros((16, CHUNK), jnp.float32))
    squares = jnp.sum(squares, axis=0, keepdims=True)
    lanes = squares[:, 0:128] + squares[:, 128:256] + squares[:, 256:384] + squares[:, 384:512]
    pair_rows[shard] = lanes

    for load in loads[1:]:
        load.wait()

    @pl.loop(0, N_DP)
    def _(j):
        base = j * PER_PEER
        rows = [send_ref[base + q] for q in range(PER_PEER)]
        for old, send in zip(olds, sends, strict=True):
            for half in range(2):
                tiles = [old[row + half * (NSEG * 8)] for row in rows]
                for q, tile in enumerate(tiles):
                    send[half * BLOCKS + base + q] = tile

    own = pl.ds(parity * BLOCKS + me * PER_PEER, PER_PEER)
    for send, recv in zip(sends, recvs, strict=True):
        recv[own] = send[own]

    pl.semaphore_wait(barrier, 130)

    for k in (1, 2, 3):
        pltpu.make_async_remote_copy(
            src_ref=pair_rows.at[shard],
            dst_ref=pair_rows.at[shard],
            send_sem=small_send.at[0],
            recv_sem=small_recv.at[0],
            device_id=(me, (shard + k) % 4),
            device_id_type=MESH,
        ).start()

    def send_all(a):
        @pl.loop(0, 127)
        def _(n):
            j, half = peer_of(n)
            pltpu.make_async_remote_copy(
                src_ref=sends[a].at[pl.ds(half * BLOCKS + j * PER_PEER, PER_PEER)],
                dst_ref=recvs[a].at[pl.ds(parity * BLOCKS + me * PER_PEER, PER_PEER)],
                send_sem=send_sem,
                recv_sem=recv_sems.at[a],
                device_id=(j, even_shard + half),
                device_id_type=MESH,
            ).start()

    send_all(0)

    three = pair_rows.at[pl.ds(0, 3)]
    pltpu.make_async_copy(three, three, small_recv.at[0]).wait()
    lanes = pair_rows[0] + pair_rows[1] + pair_rows[2] + pair_rows[3]
    own_row[0] = lanes
    all_rows[me] = lanes

    ids = lax.broadcasted_iota(jnp.int32, (RD, 128), 0) * 128 + lax.broadcasted_iota(jnp.int32, (RD, 128), 1)

    def find(n, table):
        for q in range(16):
            k = n * 16 + q
            table = jnp.where(ids == place_ref[k], k, table)
        return table

    inverse[...] = lax.fori_loop(0, BLOCKS // 16, find, jnp.zeros((RD, 128), jnp.int32))
    table_copy = pltpu.make_async_copy(inverse, inverse_smem, table_sem)
    table_copy.start()

    @pl.loop(0, 63)
    def _(n):
        j, _ = peer_of(jnp.where(n < 32, 32 + n, 64 + n))
        pltpu.make_async_remote_copy(
            src_ref=own_row.at[0],
            dst_ref=all_rows.at[me],
            send_sem=small_send.at[1],
            recv_sem=small_recv.at[1],
            device_id=(j, shard),
            device_id_type=MESH,
        ).start()

    send_all(1)
    send_all(2)
    table_copy.wait()

    def arrive(a):
        span = recvs[a].at[pl.ds(0, 127 * PER_PEER)]
        pltpu.make_async_copy(span, span, recv_sems.at[a]).wait()

        @pl.loop(0, 3 * NSEG)
        def _(n):
            group, s = n // NSEG, n % NSEG
            places = [inverse_smem[group * 16 + r, s] for r in range(16)]
            for half in range(2):
                column = pl.ds(pl.multiple_of(half * HALF + s * 128, 128), 128)
                tiles = [recvs[a][place + half * BLOCKS] for place in places]
                for r, tile in enumerate(tiles):
                    news[a][group, pl.ds(r, 1), column] = tile

    def each_chunk(body):
        @pl.loop(0, 54)
        def _(n):
            body(n // 18, pl.ds(pl.multiple_of((n % 18) * CHUNK, CHUNK), CHUNK))

    arrive(0)
    rest = all_rows.at[pl.ds(0, 63)]
    pltpu.make_async_copy(rest, rest, small_recv.at[1]).wait()
    total = all_rows[0]
    for k in range(1, N_DP):
        total = total + all_rows[k]
    sum_squares = jnp.sum(total, axis=(0, 1), keepdims=True)
    limit = clip_ratio * jnp.sqrt(jnp.float32(ROWS * FF))
    clip_scale = jnp.minimum(1.0, limit / jnp.sqrt(sum_squares + 1e-06))

    def first_step(group, columns):
        scaled = clip_scale * grad[group, :, columns].astype(jnp.float32)
        new0[group, :, columns] = beta_one * new0[group, :, columns] + (1.0 - beta_one) * scaled

    def second_step(group, columns):
        scaled = clip_scale * grad[group, :, columns].astype(jnp.float32)
        moment2 = beta_two * new1[group, :, columns] + (1.0 - beta_two) * scaled * scaled
        new1[group, :, columns] = moment2
        moment1 = new0[group, :, columns]
        update[group, :, columns] = moment1 / correct_one / (jnp.sqrt(moment2 / correct_two) + adam_eps)

    def master_step(group, columns):
        value = new2[group, :, columns]
        new2[group, :, columns] = value - learning_rate * (update[group, :, columns] + weight_decay * value)

    each_chunk(first_step)
    pltpu.make_async_copy(new0, first_out, out_sems.at[0]).start()
    arrive(1)
    each_chunk(second_step)
    pltpu.make_async_copy(new1, second_out, out_sems.at[1]).start()
    arrive(2)
    each_chunk(master_step)
    pltpu.make_async_copy(new2, master_out, out_sems.at[2]).start()

    for send in sends:
        span = send.at[pl.ds(0, 127 * PER_PEER)]
        pltpu.make_async_copy(span, span, send_sem).wait()
    pltpu.make_async_copy(three, three, small_send.at[0]).wait()
    pltpu.make_async_copy(rest, rest, small_send.at[1]).wait()
    for a in range(3):
        pltpu.make_async_copy(news[a], outs[a], out_sems.at[a]).wait()


def per_device(master_old, moment1_old, moment2_old, grad, send_slots, recv_slots):
    def rows_of(matrix):
        return matrix.reshape(RD // 8, 8, COLS // 128, 128).transpose(0, 2, 1, 3).reshape(TILES, 1, 128)

    slot = send_slots[0]
    row, segment = slot // NSEG, slot % NSEG
    send_rows = ((row // 8) * (COLS // 128) + segment) * 8 + row % 8
    slot = recv_slots[0]
    place = (slot // NSEG) * 128 + slot % NSEG
    smem = pl.BlockSpec(memory_space=pltpu.SMEM)
    hbm = pl.BlockSpec(memory_space=pl.ANY)
    tiles = pltpu.VMEM((TILES, 1, 128), jnp.float32)
    whole = pltpu.VMEM((3, 16, COLS), jnp.float32)
    new = pl.pallas_call(
        kernel,
        out_shape=[jax.ShapeDtypeStruct((3, 16, COLS), jnp.float32)] * 3,
        in_specs=[smem, smem, hbm, hbm, hbm, hbm],
        out_specs=[hbm, hbm, hbm],
        scratch_shapes=[tiles] * 9
        + [whole] * 3
        + [
            pltpu.VMEM((3, 16, COLS), jnp.bfloat16),
            whole,
            pltpu.VMEM((4, 1, 128), jnp.float32),
            pltpu.VMEM((1, 1, 128), jnp.float32),
            pltpu.VMEM((N_DP, 1, 128), jnp.float32),
            pltpu.VMEM((RD, 128), jnp.int32),
            pltpu.SMEM((RD, 128), jnp.int32),
            pltpu.SemaphoreType.DMA((4,)),
            pltpu.SemaphoreType.DMA((3,)),
            pltpu.SemaphoreType.DMA,
            pltpu.SemaphoreType.DMA((3,)),
            pltpu.SemaphoreType.DMA((2,)),
            pltpu.SemaphoreType.DMA((2,)),
            pltpu.SemaphoreType.DMA,
        ],
        compiler_params=pltpu.CompilerParams(
            collective_id=0, has_side_effects=True, vmem_limit_bytes=56 * 2**20
        ),
    )(send_rows, place, rows_of(moment1_old), rows_of(moment2_old), rows_of(master_old), grad.reshape(3, 16, COLS))
    moment1, moment2, master = [array.reshape(RD, COLS) for array in new]
    return (master, moment1, moment2)


def solution(mesh):
    specs = (P("dp", "tensor"),) * 4 + (P("dp", None),) * 2
    return jax.shard_map(
        per_device, mesh=mesh, in_specs=specs, out_specs=(P("dp", "tensor"),) * 3, check_vma=False
    )
```

```python
import functools

import jax
import jax.numpy as jnp
from jax import lax
from jax.experimental import pallas as pl
from jax.experimental.pallas import tpu as pltpu
from jax.sharding import PartitionSpec as P

ROWS = 3072
FF = 36864
SEGW = 128
RD = 48
COLS = 9216
HALF = 4608
NSEG = 36
BLOCKS = 1728
N_DP = 64
PER_PEER = 27
TILES = 2 * BLOCKS
MESH = pl.DeviceIdType.MESH

beta_one = 0.9
beta_two = 0.95
correct_one = 0.6513215599
correct_two = 0.4012630608
adam_eps = 1e-08
learning_rate = 0.01
weight_decay = 0.1
clip_ratio = 0.75

CHUNK = 512


def kernel(
    send_hbm, place_hbm, first_hbm, second_hbm, master_hbm, grad_hbm,
    new0, new1, new2, update,
    old0, old1, old2, send0, send1, send2, recv0, recv1, recv2,
    grad, pair_rows, own_row, all_rows, slots, source_rows, inverse, send_ref, place_ref, inverse_smem,
    load_sems, table_sems, send_sem, recv_sems, small_send, small_recv, entered,
):
    me = lax.axis_index("dp")
    shard = lax.axis_index("tensor")
    z, x, core = me // 8, (me // 2) % 4, me % 2
    parity = shard % 2
    partner = shard + 1 - 2 * parity
    olds, sends, recvs, news = (old0, old1, old2), (send0, send1, send2), (recv0, recv1, recv2), (new0, new1, new2)

    def dp_at(dz, dx, dc):
        return (((z + dz) % 8) * 4 + (x + dx) % 4) * 2 + (core + dc) % 2

    def signal(semaphore, j, t):
        pl.semaphore_signal(semaphore, inc=1, device_id=(j, t), device_id_type=MESH)

    barrier = pltpu.get_barrier_semaphore()
    for k in (4, 3, 5, 2, 6, 1, 7):
        signal(barrier, dp_at(k, 0, 0), shard)
    for k in (2, 1, 3):
        signal(barrier, dp_at(0, k, 0), shard)
    signal(barrier, dp_at(0, 0, 1), shard)
    for k in (1, 2, 3):
        signal(barrier, me, (shard + k) % 4)

    loads = [
        pltpu.make_async_copy(source, target, load_sems.at[k])
        for k, (source, target) in enumerate(
            [
                (send_hbm, slots),
                (first_hbm, old0),
                (second_hbm, old1),
                (master_hbm, old2),
                (grad_hbm, grad),
                (place_hbm, place_ref),
            ]
        )
    ]
    for load in loads:
        load.start()

    loads[0].wait()
    slot = slots[...]
    row = (slot * 1821) >> 16
    source_rows[...] = slot * 8 + (row >> 3) * (COLS // 128 * 8) - row * (NSEG * 8) + (row & 7)
    rows_copy = pltpu.make_async_copy(source_rows, send_ref, table_sems.at[0])
    rows_copy.start()
    for load in loads[1:5]:
        load.wait()

    def square(n, total):
        block = grad[n // 18, :, pl.ds(pl.multiple_of((n % 18) * CHUNK, CHUNK), CHUNK)].astype(jnp.float32)
        return total + block * block

    squares = lax.fori_loop(0, 54, square, jnp.zeros((16, CHUNK), jnp.float32))
    squares = jnp.sum(squares, axis=0, keepdims=True)
    pair_rows[shard] = squares[:, 0:128] + squares[:, 128:256] + squares[:, 256:384] + squares[:, 384:512]
    rows_copy.wait()

    def along_z(k):
        return jnp.where(k % 2 == 0, 4 + k // 2, 3 - k // 2)

    def offset_of(n):
        plane, other = n - 11, n - 32
        dz = jnp.where(n < 7, along_z(n), jnp.where(n < 11, 0, jnp.where(n < 32, along_z(plane % 7), along_z(other % 8))))
        dx = jnp.where(n < 7, 0, jnp.where(n < 11, (n - 6) % 4, jnp.where(n < 32, 1 + plane // 7, (other // 8 + 1) % 4)))
        dc = jnp.where(n == 10, 1, jnp.where(n < 32, 0, 1))
        return dp_at(dz % 8, dx, jnp.where(n == 63, 0, dc))

    def gather(n):
        base = offset_of(n) * PER_PEER
        rows = [send_ref[0, base + q] for q in range(PER_PEER)]
        for old, send in zip(olds, sends, strict=True):
            for half in range(2):
                tiles = [old[row + half * (NSEG * 8)] for row in rows]
                for q, tile in enumerate(tiles):
                    send[half * BLOCKS + base + q] = tile

    def deliver(a, j, t, half):
        pltpu.make_async_remote_copy(
            src_ref=sends[a].at[pl.ds(half * BLOCKS + j * PER_PEER, PER_PEER)],
            dst_ref=recvs[a].at[pl.ds(parity * BLOCKS + me * PER_PEER, PER_PEER)],
            send_sem=send_sem,
            recv_sem=recv_sems.at[a],
            device_id=(j, t),
            device_id_type=MESH,
        ).start()

    def deliver_here(a, n):
        deliver(a, offset_of(n), shard, parity)

    def deliver_partner(a, n):
        deliver(a, offset_of(n), partner, 1 - parity)

    def gather_and_deliver(first, last):
        @pl.loop(first, last)
        def _(n):
            gather(n)
            deliver_here(0, n - 1)

    EARLY = 4

    @pl.loop(0, EARLY)
    def _(n):
        gather(n)

    pl.semaphore_wait(barrier, 14)
    for k in (2, 1, 3):
        signal(entered.at[0], dp_at(0, k, 0), shard)
    for k in (1, 2, 3):
        pltpu.make_async_remote_copy(
            src_ref=pair_rows.at[shard],
            dst_ref=pair_rows.at[shard],
            send_sem=small_send.at[0],
            recv_sem=small_recv.at[0],
            device_id=(me, (shard + k) % 4),
            device_id_type=MESH,
        ).start()

    @pl.loop(0, EARLY - 1)
    def _(n):
        deliver_here(0, n)

    gather_and_deliver(EARLY, 12)
    pl.semaphore_wait(entered.at[0], 3)
    signal(entered.at[1], dp_at(0, 0, 1), shard)
    gather_and_deliver(12, 33)
    pl.semaphore_wait(entered.at[1], 1)
    signal(entered.at[2], me, partner)
    gather_and_deliver(33, 64)
    pl.semaphore_wait(entered.at[2], 1)

    @pl.loop(0, 64)
    def _(n):
        deliver_partner(0, n)

    own = pl.ds(parity * BLOCKS + me * PER_PEER, PER_PEER)
    for send, recv in zip(sends, recvs, strict=True):
        recv[own] = send[own]

    three = pair_rows.at[pl.ds(0, 3)]
    pltpu.make_async_copy(three, three, small_recv.at[0]).wait()
    lanes = pair_rows[0] + pair_rows[1] + pair_rows[2] + pair_rows[3]
    own_row[0] = lanes
    all_rows[me] = lanes

    loads[5].wait()
    lane = lax.broadcasted_iota(jnp.int32, (RD, 128), 1)
    ids = jnp.where(lane < NSEG, lax.broadcasted_iota(jnp.int32, (RD, 128), 0) * NSEG + lane, -1)

    def find(n, table):
        for q in range(16):
            k = n * 16 + q
            table = jnp.where(ids == place_ref[0, k], k, table)
        return table

    inverse[...] = lax.fori_loop(0, BLOCKS // 16, find, jnp.zeros((RD, 128), jnp.int32))
    table_copy = pltpu.make_async_copy(inverse, inverse_smem, table_sems.at[1])
    table_copy.start()

    @pl.loop(0, 63)
    def _(n):
        pltpu.make_async_remote_copy(
            src_ref=own_row.at[0],
            dst_ref=all_rows.at[me],
            send_sem=small_send.at[1],
            recv_sem=small_recv.at[1],
            device_id=(offset_of(n), shard),
            device_id_type=MESH,
        ).start()

    for a in (1, 2):

        @pl.loop(0, 63)
        def _(n):
            deliver_here(a, n)

        @pl.loop(0, 64)
        def _(n):
            deliver_partner(a, n)

    table_copy.wait()

    def arrive(a):
        span = recvs[a].at[pl.ds(0, 127 * PER_PEER)]
        pltpu.make_async_copy(span, span, recv_sems.at[a]).wait()

        @pl.loop(0, 3 * NSEG)
        def _(n):
            group, s = n // NSEG, n % NSEG
            places = [inverse_smem[group * 16 + r, s] for r in range(16)]
            for half in range(2):
                column = pl.ds(pl.multiple_of(half * HALF + s * 128, 128), 128)
                tiles = [recvs[a][place + half * BLOCKS] for place in places]
                for r, tile in enumerate(tiles):
                    news[a][group, pl.ds(r, 1), column] = tile

    def each_chunk(body):
        @pl.loop(0, 54)
        def _(n):
            body(n // 18, pl.ds(pl.multiple_of((n % 18) * CHUNK, CHUNK), CHUNK))

    arrive(0)
    rest = all_rows.at[pl.ds(0, 63)]
    pltpu.make_async_copy(rest, rest, small_recv.at[1]).wait()
    total = all_rows[0]
    for k in range(1, N_DP):
        total = total + all_rows[k]
    sum_squares = jnp.sum(total, axis=(0, 1), keepdims=True)
    limit = clip_ratio * jnp.sqrt(jnp.float32(ROWS * FF))
    clip_scale = jnp.minimum(1.0, limit / jnp.sqrt(sum_squares + 1e-06))

    def first_step(group, columns):
        scaled = clip_scale * grad[group, :, columns].astype(jnp.float32)
        new0[group, :, columns] = beta_one * new0[group, :, columns] + (1.0 - beta_one) * scaled

    def second_step(group, columns):
        scaled = clip_scale * grad[group, :, columns].astype(jnp.float32)
        moment2 = beta_two * new1[group, :, columns] + (1.0 - beta_two) * scaled * scaled
        new1[group, :, columns] = moment2
        moment1 = new0[group, :, columns]
        update[group, :, columns] = moment1 / correct_one / (jnp.sqrt(moment2 / correct_two) + adam_eps)

    each_chunk(first_step)
    arrive(1)
    each_chunk(second_step)
    for send in sends[:2]:
        span = send.at[pl.ds(0, 127 * PER_PEER)]
        pltpu.make_async_copy(span, span, send_sem).wait()
    pltpu.make_async_copy(three, three, small_send.at[0]).wait()
    pltpu.make_async_copy(rest, rest, small_send.at[1]).wait()
    arrive(2)
    span = send2.at[pl.ds(0, 127 * PER_PEER)]
    pltpu.make_async_copy(span, span, send_sem).wait()


def finish(new0, new1, new2, update, first_out, second_out, master_out, master, sems):
    copies = [
        pltpu.make_async_copy(new0, first_out, sems.at[0]),
        pltpu.make_async_copy(new1, second_out, sems.at[1]),
    ]
    for copy in copies:
        copy.start()
    for group in range(3):

        @pl.loop(0, COLS // CHUNK)
        def _(n):
            columns = pl.ds(pl.multiple_of(n * CHUNK, CHUNK), CHUNK)
            value = new2[group, :, columns]
            master[group, :, columns] = value - learning_rate * (update[group, :, columns] + weight_decay * value)

        copy = pltpu.make_async_copy(master.at[group], master_out.at[group], sems.at[2 + group])
        copy.start()
        copies.append(copy)
    for copy in copies:
        copy.wait()


def per_device(master_old, moment1_old, moment2_old, grad, send_slots, recv_slots):
    def rows_of(matrix):
        return matrix.reshape(RD // 8, 8, COLS // 128, 128).transpose(0, 2, 1, 3).reshape(TILES, 1, 128)

    hbm = pl.BlockSpec(memory_space=pl.ANY)
    tiles = pltpu.VMEM((TILES, 1, 128), jnp.float32)
    whole = pltpu.VMEM((3, 16, COLS), jnp.float32)
    vmem = pl.BlockSpec(memory_space=pltpu.VMEM)
    kept = pl.pallas_call(
        kernel,
        out_shape=[pltpu.VMEM((3, 16, COLS), jnp.float32)] * 4,
        in_specs=[hbm] * 6,
        out_specs=[vmem] * 4,
        scratch_shapes=[tiles] * 9
        + [
            pltpu.VMEM((3, 16, COLS), jnp.bfloat16),
            pltpu.VMEM((4, 1, 128), jnp.float32),
            pltpu.VMEM((1, 1, 128), jnp.float32),
            pltpu.VMEM((N_DP, 1, 128), jnp.float32),
            pltpu.VMEM((1, BLOCKS), jnp.int32),
            pltpu.VMEM((1, BLOCKS), jnp.int32),
            pltpu.VMEM((RD, 128), jnp.int32),
            pltpu.SMEM((1, BLOCKS), jnp.int32),
            pltpu.SMEM((1, BLOCKS), jnp.int32),
            pltpu.SMEM((RD, 128), jnp.int32),
            pltpu.SemaphoreType.DMA((6,)),
            pltpu.SemaphoreType.DMA((2,)),
            pltpu.SemaphoreType.DMA,
            pltpu.SemaphoreType.DMA((3,)),
            pltpu.SemaphoreType.DMA((2,)),
            pltpu.SemaphoreType.DMA((2,)),
            pltpu.SemaphoreType.REGULAR((3,)),
        ],
        compiler_params=pltpu.CompilerParams(
            collective_id=0, has_side_effects=True, vmem_limit_bytes=57 * 2**20
        ),
    )(send_slots, recv_slots, rows_of(moment1_old), rows_of(moment2_old), rows_of(master_old), grad.reshape(3, 16, COLS))
    new = pl.pallas_call(
        finish,
        out_shape=[jax.ShapeDtypeStruct((3, 16, COLS), jnp.float32)] * 3,
        in_specs=[vmem] * 4,
        out_specs=[hbm] * 3,
        scratch_shapes=[pltpu.VMEM((3, 16, COLS), jnp.float32), pltpu.SemaphoreType.DMA((5,))],
        compiler_params=pltpu.CompilerParams(vmem_limit_bytes=16 * 2**20),
    )(*kept)
    moment1, moment2, master = [array.reshape(RD, COLS) for array in new]
    return (master, moment1, moment2)


def solution(mesh):
    specs = (P("dp", "tensor"),) * 4 + (P("dp", None),) * 2
    return jax.shard_map(
        per_device, mesh=mesh, in_specs=specs, out_specs=(P("dp", "tensor"),) * 3, check_vma=False
    )
```

```python
import functools

import jax
import jax.numpy as jnp
from jax import lax
from jax.experimental import pallas as pl
from jax.experimental.pallas import tpu as pltpu
from jax.sharding import PartitionSpec as P

ROWS = 3072
FF = 36864
SEGW = 128
RD = 48
COLS = 9216
HALF = 4608
NSEG = 36
BLOCKS = 1728
N_DP = 64
PER_PEER = 27
TILES = 2 * BLOCKS
MESH = pl.DeviceIdType.MESH

beta_one = 0.9
beta_two = 0.95
correct_one = 0.6513215599
correct_two = 0.4012630608
adam_eps = 1e-08
learning_rate = 0.01
weight_decay = 0.1
clip_ratio = 0.75

CHUNK = 512
EARLY = 3


def kernel(
    send_hbm, place_hbm, first_hbm, second_hbm, master_hbm, grad_hbm,
    new0, new1, update, recv2, inverse,
    old0, old1, old2, send0, send1, send2, recv0, recv1,
    grad, shard_rows, line_rows, plane_rows, slots, source_rows, send_ref, place_ref, inverse_smem,
    load_sems, table_sems, send_sem, recv_sems, small_send, small_recv, entered,
):
    me = lax.axis_index("dp")
    shard = lax.axis_index("tensor")
    z, x, core = me // 8, (me // 2) % 4, me % 2
    parity = shard % 2
    partner = shard + 1 - 2 * parity
    olds, sends, recvs = (old0, old1, old2), (send0, send1, send2), (recv0, recv1, recv2)

    def dp_at(dz, dx, dc):
        return (((z + dz) % 8) * 4 + (x + dx) % 4) * 2 + (core + dc) % 2

    def signal(semaphore, j, t):
        pl.semaphore_signal(semaphore, inc=1, device_id=(j, t), device_id_type=MESH)

    barrier = pltpu.get_barrier_semaphore()
    for k in (4, 3, 5, 2, 6, 1, 7):
        signal(barrier, dp_at(k, 0, 0), shard)
    for k in (2, 1, 3):
        signal(barrier, dp_at(0, k, 0), shard)
    signal(barrier, dp_at(0, 0, 1), shard)
    for k in (1, 2, 3):
        signal(barrier, me, (shard + k) % 4)

    loads = [
        pltpu.make_async_copy(source, target, load_sems.at[k])
        for k, (source, target) in enumerate(
            [
                (send_hbm, slots),
                (first_hbm, old0),
                (second_hbm, old1),
                (master_hbm, old2),
                (grad_hbm, grad),
                (place_hbm, place_ref),
            ]
        )
    ]
    for load in loads:
        load.start()

    loads[0].wait()
    slot = slots[...]
    row = (slot * 1821) >> 16
    source_rows[...] = slot * 8 + (row >> 3) * (COLS // 128 * 8) - row * (NSEG * 8) + (row & 7)
    rows_copy = pltpu.make_async_copy(source_rows, send_ref, table_sems.at[0])
    rows_copy.start()

    def offset_of(n):
        zi = n & 7
        dz = jnp.where((zi & 1) == 0, 4 + (zi >> 1), 3 - (zi >> 1))
        return (((z + dz) & 7) << 3) + (((x + (n >> 3)) & 3) << 1) + ((core + (n >> 5)) & 1)

    def gather(a, n):
        base = offset_of(n) * PER_PEER
        rows = [send_ref[0, base + q] for q in range(PER_PEER)]
        for half in range(2):
            tiles = [olds[a][row + half * (NSEG * 8)] for row in rows]
            for q, tile in enumerate(tiles):
                sends[a][half * BLOCKS + base + q] = tile

    def deliver(a, j, t, half):
        pltpu.make_async_remote_copy(
            src_ref=sends[a].at[pl.ds(half * BLOCKS + j * PER_PEER, PER_PEER)],
            dst_ref=recvs[a].at[pl.ds(parity * BLOCKS + me * PER_PEER, PER_PEER)],
            send_sem=send_sem,
            recv_sem=recv_sems.at[a],
            device_id=(j, t),
            device_id_type=MESH,
        ).start()

    def deliver_here(a, n):
        deliver(a, offset_of(n), shard, parity)

    def deliver_partner(a, n):
        deliver(a, offset_of(n), partner, 1 - parity)

    def gather_and_deliver(first, last):
        @pl.loop(first, last)
        def _(n):
            gather(0, n)
            deliver_here(0, n - 1)

    rows_copy.wait()
    loads[1].wait()

    @pl.loop(0, EARLY)
    def _(n):
        gather(0, n)

    pl.semaphore_wait(barrier, 14)
    for k in (2, 1, 3):
        signal(entered.at[0], dp_at(0, k, 0), shard)

    @pl.loop(0, EARLY - 1)
    def _(n):
        deliver_here(0, n)

    gather_and_deliver(EARLY, 8)
    gather(0, 8)
    pl.semaphore_wait(entered.at[0], 3)
    signal(entered.at[1], dp_at(0, 0, 1), shard)
    gather_and_deliver(9, 33)
    pl.semaphore_wait(entered.at[1], 1)
    signal(entered.at[2], me, partner)
    gather_and_deliver(33, 64)
    pl.semaphore_wait(entered.at[2], 1)

    @pl.loop(0, 64)
    def _(n):
        deliver_partner(0, n)

    deliver_here(0, 63)

    loads[4].wait()

    def square(n, total):
        group = jnp.where(n >= 18, 1, 0) + jnp.where(n >= 36, 1, 0)
        columns = pl.ds(pl.multiple_of((n - 18 * group) * CHUNK, CHUNK), CHUNK)
        block = grad[group, :, columns].astype(jnp.float32)
        return total + block * block

    squares = lax.fori_loop(0, 54, square, jnp.zeros((16, CHUNK), jnp.float32))
    squares = jnp.sum(squares, axis=0, keepdims=True)
    shard_rows[shard] = squares[:, 0:128] + squares[:, 128:256] + squares[:, 256:384] + squares[:, 384:512]

    def pass_row(k, rows, own, j, t):
        pltpu.make_async_remote_copy(
            src_ref=rows.at[own],
            dst_ref=rows.at[own],
            send_sem=small_send.at[k],
            recv_sem=small_recv.at[k],
            device_id=(j, t),
            device_id_type=MESH,
        ).start()

    def wait_rows(rows, semaphore):
        others = rows.at[pl.ds(0, rows.shape[0] - 1)]
        pltpu.make_async_copy(others, others, semaphore).wait()

    def sum_of(rows):
        total = rows[0]
        for k in range(1, rows.shape[0]):
            total = total + rows[k]
        return total

    def gather_all(a):
        @pl.loop(0, 64)
        def _(n):
            gather(a, n)

        own = pl.ds(parity * BLOCKS + me * PER_PEER, PER_PEER)
        recvs[a][own] = sends[a][own]

    def deliver_all(a):
        def peer(n):
            zi, xi = n & 7, (n >> 3) & 3
            dz = jnp.where((zi & 1) == 0, 4 + (zi >> 1), 3 - (zi >> 1))
            dx = jnp.where(xi == 0, 2, jnp.where(xi == 3, 0, 2 * xi - 1))
            return (((z + dz) & 7) << 3) + (((x + dx) & 3) << 1) + ((core + 1 - (n >> 5)) & 1)

        @pl.loop(0, 63)
        def _(n):
            deliver(a, peer(n), shard, parity)
            deliver(a, peer(n), partner, 1 - parity)

        deliver(a, me, partner, 1 - parity)

    own = pl.ds(parity * BLOCKS + me * PER_PEER, PER_PEER)
    recv0[own] = send0[own]
    loads[2].wait()
    gather_all(1)
    for k in (1, 2, 3):
        pass_row(0, shard_rows, shard, me, (shard + k) % 4)
    loads[3].wait()
    gather_all(2)
    wait_rows(shard_rows, small_recv.at[0])
    line_rows[z * 2 + core] = sum_of(shard_rows)

    loads[5].wait()
    line = lax.broadcasted_iota(jnp.int32, (16, 128), 0)
    lane = lax.broadcasted_iota(jnp.int32, (16, 128), 1)
    group = jnp.where(line >= 5, 1, 0) + jnp.where(line >= 10, 1, 0)
    segment = (line - 5 * group) * 8 + (lane >> 4)
    ids = jnp.where((segment < NSEG) & (line < 15), (group * 16 + (lane & 15)) * NSEG + segment, -1)

    def find(n, table):
        for q in range(16):
            k = n * 16 + q
            table = jnp.where(ids == place_ref[0, k], k, table)
        return table

    inverse[...] = lax.fori_loop(0, BLOCKS // 16, find, jnp.zeros((16, 128), jnp.int32))
    table_copy = pltpu.make_async_copy(inverse, inverse_smem, table_sems.at[1])
    table_copy.start()

    for k in range(1, 16):
        pass_row(1, line_rows, z * 2 + core, dp_at(k >> 1, 0, k & 1), shard)
    deliver_all(1)
    table_copy.wait()

    def arrive(a, new):
        span = recvs[a].at[pl.ds(0, 127 * PER_PEER)]
        pltpu.make_async_copy(span, span, recv_sems.at[a]).wait()

        @pl.loop(0, 12)
        def _(n):
            place(recvs[a], inverse_smem, new, (n >> 2) * 5 + (n & 3), n >> 2, (n & 3) * 8, 8)

        @pl.loop(0, 3)
        def _(n):
            place(recvs[a], inverse_smem, new, n * 5 + 4, n, 32, 4)

    def each_chunk(body):
        @pl.loop(0, 54)
        def _(n):
            group = jnp.where(n >= 18, 1, 0) + jnp.where(n >= 36, 1, 0)
            body(group, pl.ds(pl.multiple_of((n - 18 * group) * CHUNK, CHUNK), CHUNK))

    wait_rows(line_rows, small_recv.at[1])
    plane_rows[x] = sum_of(line_rows)
    arrive(0, new0)
    for k in (1, 2, 3):
        pass_row(2, plane_rows, x, dp_at(0, k, 0), shard)
    deliver_all(2)
    arrive(1, new1)

    wait_rows(plane_rows, small_recv.at[2])
    total = sum_of(plane_rows)
    sum_squares = jnp.sum(total, axis=(0, 1), keepdims=True)
    limit = clip_ratio * jnp.sqrt(jnp.float32(ROWS * FF))
    clip_scale = jnp.minimum(1.0, limit / jnp.sqrt(sum_squares + 1e-06))

    def first_step(group, columns):
        scaled = clip_scale * grad[group, :, columns].astype(jnp.float32)
        new0[group, :, columns] = beta_one * new0[group, :, columns] + (1.0 - beta_one) * scaled

    def second_step(group, columns):
        scaled = clip_scale * grad[group, :, columns].astype(jnp.float32)
        moment2 = beta_two * new1[group, :, columns] + (1.0 - beta_two) * scaled * scaled
        new1[group, :, columns] = moment2
        moment1 = new0[group, :, columns]
        update[group, :, columns] = moment1 / correct_one / (jnp.sqrt(moment2 / correct_two) + adam_eps)

    each_chunk(first_step)
    each_chunk(second_step)
    for rows, semaphore in zip((shard_rows, line_rows, plane_rows), range(3), strict=True):
        wait_rows(rows, small_send.at[semaphore])
    for a in range(3):
        span = sends[a].at[pl.ds(0, 127 * PER_PEER)]
        pltpu.make_async_copy(span, span, send_sem).wait()
    span = recv2.at[pl.ds(0, 127 * PER_PEER)]
    pltpu.make_async_copy(span, span, recv_sems.at[2]).wait()


def place(recv, inverse, new, line, group, segment, count):
    for u in range(count):
        tiles = []
        for r in range(16):
            source = inverse[line, u * 16 + r]
            tiles.append((recv[source], recv[source + BLOCKS]))
        for half in range(2):
            column = pl.ds(pl.multiple_of((half * NSEG + segment + u) * 128, 128), 128)
            for r in range(16):
                new[group, pl.ds(r, 1), column] = tiles[r][half]


def finish(new0, new1, update, recv2, inverse, first_out, second_out, master_out, master, inverse_smem, sems):
    table = pltpu.make_async_copy(inverse, inverse_smem, sems.at[5])
    table.start()
    copies = [
        pltpu.make_async_copy(new0, first_out, sems.at[0]),
        pltpu.make_async_copy(new1, second_out, sems.at[1]),
    ]
    for copy in copies:
        copy.start()
    table.wait()
    for group in range(3):

        @pl.loop(0, 4)
        def _(n):
            place(recv2, inverse_smem, master, group * 5 + n, group, n * 8, 8)

        place(recv2, inverse_smem, master, group * 5 + 4, group, 32, 4)

        @pl.loop(0, COLS // CHUNK)
        def _(n):
            columns = pl.ds(pl.multiple_of(n * CHUNK, CHUNK), CHUNK)
            value = master[group, :, columns]
            master[group, :, columns] = value - learning_rate * (update[group, :, columns] + weight_decay * value)

        copy = pltpu.make_async_copy(master.at[group], master_out.at[group], sems.at[2 + group])
        copy.start()
        copies.append(copy)
    for copy in copies:
        copy.wait()


def per_device(master_old, moment1_old, moment2_old, grad, send_slots, recv_slots):
    def rows_of(matrix):
        return matrix.reshape(RD // 8, 8, COLS // 128, 128).transpose(0, 2, 1, 3).reshape(TILES, 1, 128)

    hbm = pl.BlockSpec(memory_space=pl.ANY)
    tiles = pltpu.VMEM((TILES, 1, 128), jnp.float32)
    whole = pltpu.VMEM((3, 16, COLS), jnp.float32)
    vmem = pl.BlockSpec(memory_space=pltpu.VMEM)
    kept = pl.pallas_call(
        kernel,
        out_shape=[whole] * 3 + [tiles, pltpu.VMEM((16, 128), jnp.int32)],
        in_specs=[hbm] * 6,
        out_specs=[vmem] * 5,
        scratch_shapes=[tiles] * 8
        + [
            pltpu.VMEM((3, 16, COLS), jnp.bfloat16),
            pltpu.VMEM((4, 1, 128), jnp.float32),
            pltpu.VMEM((16, 1, 128), jnp.float32),
            pltpu.VMEM((4, 1, 128), jnp.float32),
            pltpu.VMEM((1, BLOCKS), jnp.int32),
            pltpu.VMEM((1, BLOCKS), jnp.int32),
            pltpu.SMEM((1, BLOCKS), jnp.int32),
            pltpu.SMEM((1, BLOCKS), jnp.int32),
            pltpu.SMEM((16, 128), jnp.int32),
            pltpu.SemaphoreType.DMA((6,)),
            pltpu.SemaphoreType.DMA((2,)),
            pltpu.SemaphoreType.DMA,
            pltpu.SemaphoreType.DMA((3,)),
            pltpu.SemaphoreType.DMA((3,)),
            pltpu.SemaphoreType.DMA((3,)),
            pltpu.SemaphoreType.REGULAR((3,)),
        ],
        compiler_params=pltpu.CompilerParams(
            collective_id=0, has_side_effects=True, vmem_limit_bytes=57 * 2**20
        ),
    )(send_slots, recv_slots, rows_of(moment1_old), rows_of(moment2_old), rows_of(master_old), grad.reshape(3, 16, COLS))
    new = pl.pallas_call(
        finish,
        out_shape=[jax.ShapeDtypeStruct((3, 16, COLS), jnp.float32)] * 3,
        in_specs=[vmem] * 5,
        out_specs=[hbm] * 3,
        scratch_shapes=[whole, pltpu.SMEM((16, 128), jnp.int32), pltpu.SemaphoreType.DMA((6,))],
        compiler_params=pltpu.CompilerParams(vmem_limit_bytes=16 * 2**20),
    )(*kept)
    moment1, moment2, master = [array.reshape(RD, COLS) for array in new]
    return (master, moment1, moment2)


def solution(mesh):
    specs = (P("dp", "tensor"),) * 4 + (P("dp", None),) * 2
    return jax.shard_map(
        per_device, mesh=mesh, in_specs=specs, out_specs=(P("dp", "tensor"),) * 3, check_vma=False
    )
```

```python
import functools

import jax
import jax.numpy as jnp
from jax import lax
from jax.experimental import pallas as pl
from jax.experimental.pallas import tpu as pltpu
from jax.sharding import PartitionSpec as P

ROWS = 3072
FF = 36864
SEGW = 128
RD = 48
COLS = 9216
HALF = 4608
NSEG = 36
BLOCKS = 1728
N_DP = 64
PER_PEER = 27
TILES = 2 * BLOCKS
MESH = pl.DeviceIdType.MESH

beta_one = 0.9
beta_two = 0.95
correct_one = 0.6513215599
correct_two = 0.4012630608
adam_eps = 1e-08
learning_rate = 0.01
weight_decay = 0.1
clip_ratio = 0.75

CHUNK = 512
EARLY = 3
FRONT = 21
BACK = PER_PEER - FRONT


def kernel(
    send_hbm, place_hbm, first_hbm, second_hbm, master_hbm, grad_hbm,
    new0, new1, new2, update, back, back_rows,
    old0, old1, old2, send0, send1, send2, recv0, recv1, front,
    grad, shard_rows, line_rows, plane_rows, slots, inverses, send_ref, place_ref, inverse_smem, front_smem,
    load_sems, table_sems, send_sem, recv_sems, small_send, small_recv, entered,
):
    me = lax.axis_index("dp")
    shard = lax.axis_index("tensor")
    z, x, core = me // 8, (me // 2) % 4, me % 2
    parity = shard % 2
    partner = shard + 1 - 2 * parity
    olds, sends = (old0, old1, old2), (send0, send1, send2)

    def dp_at(dz, dx, dc):
        return (((z + dz) % 8) * 4 + (x + dx) % 4) * 2 + (core + dc) % 2

    def signal(semaphore, j, t):
        pl.semaphore_signal(semaphore, inc=1, device_id=(j, t), device_id_type=MESH)

    barrier = pltpu.get_barrier_semaphore()
    for k in (4, 3, 5, 2, 6, 1, 7):
        signal(barrier, dp_at(k, 0, 0), shard)
    for k in (2, 1, 3):
        signal(barrier, dp_at(0, k, 0), shard)
    signal(barrier, dp_at(0, 0, 1), shard)
    for k in (1, 2, 3):
        signal(barrier, me, (shard + k) % 4)

    loads = [
        pltpu.make_async_copy(source, target, load_sems.at[k])
        for k, (source, target) in enumerate(
            [
                (send_hbm, send_ref),
                (first_hbm, old0),
                (second_hbm, old1),
                (master_hbm, old2),
                (grad_hbm, grad),
                (place_hbm, place_ref),
                (place_hbm, slots),
            ]
        )
    ]
    for load in loads:
        load.start()

    def offset_of(n):
        zi = n & 7
        dz = jnp.where((zi & 1) == 0, 4 + (zi >> 1), 3 - (zi >> 1))
        return (((z + dz) & 7) << 3) + (((x + (n >> 3)) & 3) << 1) + ((core + (n >> 5)) & 1)

    def gather(a, n):
        base = offset_of(n) * PER_PEER
        rows = [row_of(send_ref[0, base + q]) for q in range(PER_PEER)]
        for half in range(2):
            tiles = [olds[a][row + half * (NSEG * 8)] for row in rows]
            for q, tile in enumerate(tiles):
                sends[a][half * BLOCKS + base + q] = tile

    def deliver(a, j, t, half, target, first=0, count=PER_PEER):
        pltpu.make_async_remote_copy(
            src_ref=sends[min(a, 2)].at[pl.ds(half * BLOCKS + j * PER_PEER + first, count)],
            dst_ref=target.at[pl.ds((parity * N_DP + me) * count, count)],
            send_sem=send_sem,
            recv_sem=recv_sems.at[a],
            device_id=(j, t),
            device_id_type=MESH,
        ).start()

    def deliver_here(a, n):
        deliver(a, offset_of(n), shard, parity, recv0)

    def deliver_partner(a, n):
        deliver(a, offset_of(n), partner, 1 - parity, recv0)

    def gather_and_deliver(first, last):
        @pl.loop(first, last)
        def _(n):
            gather(0, n)
            deliver_here(0, n - 1)

    loads[0].wait()
    loads[1].wait()

    @pl.loop(0, EARLY)
    def _(n):
        gather(0, n)

    pl.semaphore_wait(barrier, 14)
    for k in (2, 1, 3):
        signal(entered.at[0], dp_at(0, k, 0), shard)

    @pl.loop(0, EARLY - 1)
    def _(n):
        deliver_here(0, n)

    gather_and_deliver(EARLY, 8)
    gather(0, 8)
    pl.semaphore_wait(entered.at[0], 3)
    signal(entered.at[1], dp_at(0, 0, 1), shard)
    gather_and_deliver(9, 33)
    pl.semaphore_wait(entered.at[1], 1)
    signal(entered.at[2], me, partner)
    gather_and_deliver(33, 64)
    pl.semaphore_wait(entered.at[2], 1)

    @pl.loop(0, 64)
    def _(n):
        deliver_partner(0, n)

    deliver_here(0, 63)

    loads[4].wait()

    def square(n, total):
        group = jnp.where(n >= 18, 1, 0) + jnp.where(n >= 36, 1, 0)
        columns = pl.ds(pl.multiple_of((n - 18 * group) * CHUNK, CHUNK), CHUNK)
        block = grad[group, :, columns].astype(jnp.float32)
        return total + block * block

    squares = lax.fori_loop(0, 54, square, jnp.zeros((16, CHUNK), jnp.float32))
    squares = jnp.sum(squares, axis=0, keepdims=True)
    shard_rows[shard] = squares[:, 0:128] + squares[:, 128:256] + squares[:, 256:384] + squares[:, 384:512]

    def pass_row(k, rows, own, j, t):
        pltpu.make_async_remote_copy(
            src_ref=rows.at[own],
            dst_ref=rows.at[own],
            send_sem=small_send.at[k],
            recv_sem=small_recv.at[k],
            device_id=(j, t),
            device_id_type=MESH,
        ).start()

    def wait_rows(rows, semaphore):
        others = rows.at[pl.ds(0, rows.shape[0] - 1)]
        pltpu.make_async_copy(others, others, semaphore).wait()

    def sum_of(rows):
        total = rows[0]
        for k in range(1, rows.shape[0]):
            total = total + rows[k]
        return total

    def gather_all(a):
        @pl.loop(0, 64)
        def _(n):
            gather(a, n)

    def deliver_all(a, *place):
        def peer(n):
            zi, xi = n & 7, (n >> 3) & 3
            dz = jnp.where((zi & 1) == 0, 4 + (zi >> 1), 3 - (zi >> 1))
            dx = jnp.where(xi == 0, 2, jnp.where(xi == 3, 0, 2 * xi - 1))
            return (((z + dz) & 7) << 3) + (((x + dx) & 3) << 1) + ((core + 1 - (n >> 5)) & 1)

        @pl.loop(0, 63)
        def _(n):
            deliver(a, peer(n), shard, parity, *place)
            deliver(a, peer(n), partner, 1 - parity, *place)

        deliver(a, me, partner, 1 - parity, *place)

    def keep(send, target, first=0, count=PER_PEER):
        target[pl.ds((parity * N_DP + me) * count, count)] = send[
            pl.ds(parity * BLOCKS + me * PER_PEER + first, count)
        ]

    keep(send0, recv0)
    loads[2].wait()
    gather_all(1)
    keep(send1, recv1)
    for k in (1, 2, 3):
        pass_row(0, shard_rows, shard, me, (shard + k) % 4)
    loads[3].wait()
    gather_all(2)
    keep(send2, front, 0, FRONT)
    keep(send2, back, FRONT, BACK)
    wait_rows(shard_rows, small_recv.at[0])
    line_rows[z * 2 + core] = sum_of(shard_rows)

    loads[5].wait()
    line = lax.broadcasted_iota(jnp.int32, (16, 128), 0)
    lane = lax.broadcasted_iota(jnp.int32, (16, 128), 1)
    group = jnp.where(line >= 5, 1, 0) + jnp.where(line >= 10, 1, 0)
    segment = (line - 5 * group) * 8 + (lane >> 4)
    ids = jnp.where((segment < NSEG) & (line < 15), (group * 16 + (lane & 15)) * NSEG + segment, -1)

    def find(i, tables):
        whole, part = tables
        for q in range(PER_PEER):
            k = i * PER_PEER + q
            here = ids == place_ref[0, k]
            whole = jnp.where(here, k, whole)
            if q < FRONT:
                part = jnp.where(here, i * FRONT + q, part)
        return whole, part

    zeros = jnp.zeros((16, 128), jnp.int32)
    whole, part = lax.fori_loop(0, N_DP, find, (zeros, zeros))
    inverses[0] = whole
    inverses[1] = part
    loads[6].wait()
    back_rows[...] = row_of(slots[...])
    table_copies = [
        pltpu.make_async_copy(inverses.at[0], inverse_smem, table_sems.at[0]),
        pltpu.make_async_copy(inverses.at[1], front_smem, table_sems.at[1]),
    ]
    for copy in table_copies:
        copy.start()

    for k in range(1, 16):
        pass_row(1, line_rows, z * 2 + core, dp_at(k >> 1, 0, k & 1), shard)
    deliver_all(1, recv1)
    for copy in table_copies:
        copy.wait()

    def arrive(a, recv, table, new):
        span = recv.at[pl.ds(0, recv.shape[0] * 127 // 128)]
        pltpu.make_async_copy(span, span, recv_sems.at[a]).wait()

        @pl.loop(0, 12)
        def _(n):
            place(recv, table, new, (n >> 2) * 5 + (n & 3), n >> 2, (n & 3) * 8, 8)

        @pl.loop(0, 3)
        def _(n):
            place(recv, table, new, n * 5 + 4, n, 32, 4)

    def each_chunk(body):
        @pl.loop(0, 54)
        def _(n):
            group = jnp.where(n >= 18, 1, 0) + jnp.where(n >= 36, 1, 0)
            body(group, pl.ds(pl.multiple_of((n - 18 * group) * CHUNK, CHUNK), CHUNK))

    wait_rows(line_rows, small_recv.at[1])
    plane_rows[x] = sum_of(line_rows)
    arrive(0, recv0, inverse_smem, new0)
    for k in (1, 2, 3):
        pass_row(2, plane_rows, x, dp_at(0, k, 0), shard)
    deliver_all(2, front, 0, FRONT)
    deliver_all(3, back, FRONT, BACK)
    arrive(1, recv1, inverse_smem, new1)

    wait_rows(plane_rows, small_recv.at[2])
    total = sum_of(plane_rows)
    sum_squares = jnp.sum(total, axis=(0, 1), keepdims=True)
    limit = clip_ratio * jnp.sqrt(jnp.float32(ROWS * FF))
    clip_scale = jnp.minimum(1.0, limit / jnp.sqrt(sum_squares + 1e-06))

    def first_step(group, columns):
        scaled = clip_scale * grad[group, :, columns].astype(jnp.float32)
        new0[group, :, columns] = beta_one * new0[group, :, columns] + (1.0 - beta_one) * scaled

    def second_step(group, columns):
        scaled = clip_scale * grad[group, :, columns].astype(jnp.float32)
        moment2 = beta_two * new1[group, :, columns] + (1.0 - beta_two) * scaled * scaled
        new1[group, :, columns] = moment2
        moment1 = new0[group, :, columns]
        update[group, :, columns] = moment1 / correct_one / (jnp.sqrt(moment2 / correct_two) + adam_eps)

    each_chunk(first_step)
    each_chunk(second_step)
    arrive(2, front, front_smem, new2)
    for rows, semaphore in zip((shard_rows, line_rows, plane_rows), range(3), strict=True):
        wait_rows(rows, small_send.at[semaphore])
    for a in range(3):
        span = sends[a].at[pl.ds(0, 127 * PER_PEER)]
        pltpu.make_async_copy(span, span, send_sem).wait()
    span = back.at[pl.ds(0, 127 * BACK)]
    pltpu.make_async_copy(span, span, recv_sems.at[3]).wait()


def row_of(slot):
    row = (slot * 1821) >> 16
    return slot * 8 + (row >> 3) * (COLS // 128 * 8) - row * (NSEG * 8) + (row & 7)


def place(recv, inverse, new, line, group, segment, count):
    for u in range(count):
        tiles = []
        for r in range(16):
            source = inverse[line, u * 16 + r]
            tiles.append((recv[source], recv[source + recv.shape[0] // 2]))
        for half in range(2):
            column = pl.ds(pl.multiple_of((half * NSEG + segment + u) * 128, 128), 128)
            for r in range(16):
                new[group, pl.ds(r, 1), column] = tiles[r][half]


def finish(new0, new1, new2, update, back, back_rows, first_out, second_out, master_out, master, rows_smem, sems):
    table = pltpu.make_async_copy(back_rows, rows_smem, sems.at[5])
    table.start()
    copies = [
        pltpu.make_async_copy(new0, first_out, sems.at[0]),
        pltpu.make_async_copy(new1, second_out, sems.at[1]),
    ]
    for copy in copies:
        copy.start()

    @pl.loop(0, TILES // 128)
    def _(n):
        rows = pl.ds(pl.multiple_of(n * 128, 128), 128)
        master[rows, :] = new2[rows, :]

    table.wait()

    @pl.loop(0, N_DP // 4)
    def _(n):
        for u in range(4):
            i = n * 4 + u
            rows = [rows_smem[0, i * PER_PEER + FRONT + q] for q in range(BACK)]
            for half in range(2):
                tiles = [back[pl.ds((half * N_DP + i) * BACK + q, 1), :] for q in range(BACK)]
                for row, tile in zip(rows, tiles, strict=True):
                    master[pl.ds(row + half * (NSEG * 8), 1), :] = tile

    third = TILES // 3
    for group in range(3):

        @pl.loop(0, third // 128)
        def _(n):
            rows = pl.ds(pl.multiple_of(group * third + n * 128, 128), 128)
            value = master[rows, :]
            master[rows, :] = value - learning_rate * (update[rows, :] + weight_decay * value)

        span = pl.ds(group * third, third)
        copy = pltpu.make_async_copy(master.at[span], master_out.at[span], sems.at[2 + group])
        copy.start()
        copies.append(copy)
    for copy in copies:
        copy.wait()


def per_device(master_old, moment1_old, moment2_old, grad, send_slots, recv_slots):
    def rows_of(matrix):
        return matrix.reshape(RD // 8, 8, COLS // 128, 128).transpose(0, 2, 1, 3).reshape(TILES, 1, 128)

    hbm = pl.BlockSpec(memory_space=pl.ANY)
    tiles = pltpu.VMEM((TILES, 1, 128), jnp.float32)
    whole = pltpu.VMEM((3, 16, COLS), jnp.float32)
    vmem = pl.BlockSpec(memory_space=pltpu.VMEM)
    new0, new1, new2, update, back, back_rows = pl.pallas_call(
        kernel,
        out_shape=[whole] * 4
        + [pltpu.VMEM((2 * N_DP * BACK, 1, 128), jnp.float32), pltpu.VMEM((1, BLOCKS), jnp.int32)],
        in_specs=[hbm] * 6,
        out_specs=[vmem] * 6,
        scratch_shapes=[tiles] * 8
        + [
            pltpu.VMEM((2 * N_DP * FRONT, 1, 128), jnp.float32),
            pltpu.VMEM((3, 16, COLS), jnp.bfloat16),
            pltpu.VMEM((4, 1, 128), jnp.float32),
            pltpu.VMEM((16, 1, 128), jnp.float32),
            pltpu.VMEM((4, 1, 128), jnp.float32),
            pltpu.VMEM((1, BLOCKS), jnp.int32),
            pltpu.VMEM((2, 16, 128), jnp.int32),
            pltpu.SMEM((1, BLOCKS), jnp.int32),
            pltpu.SMEM((1, BLOCKS), jnp.int32),
            pltpu.SMEM((16, 128), jnp.int32),
            pltpu.SMEM((16, 128), jnp.int32),
            pltpu.SemaphoreType.DMA((7,)),
            pltpu.SemaphoreType.DMA((2,)),
            pltpu.SemaphoreType.DMA,
            pltpu.SemaphoreType.DMA((4,)),
            pltpu.SemaphoreType.DMA((3,)),
            pltpu.SemaphoreType.DMA((3,)),
            pltpu.SemaphoreType.REGULAR((3,)),
        ],
        compiler_params=pltpu.CompilerParams(
            collective_id=0, has_side_effects=True, vmem_limit_bytes=56 * 2**20
        ),
    )(send_slots, recv_slots, rows_of(moment1_old), rows_of(moment2_old), rows_of(master_old), grad.reshape(3, 16, COLS))
    new = pl.pallas_call(
        finish,
        out_shape=[jax.ShapeDtypeStruct((3, 16, COLS), jnp.float32)] * 2
        + [jax.ShapeDtypeStruct((TILES, 128), jnp.float32)],
        in_specs=[vmem] * 6,
        out_specs=[hbm] * 3,
        scratch_shapes=[
            pltpu.VMEM((TILES, 128), jnp.float32),
            pltpu.SMEM((1, BLOCKS), jnp.int32),
            pltpu.SemaphoreType.DMA((6,)),
        ],
        compiler_params=pltpu.CompilerParams(vmem_limit_bytes=16 * 2**20),
    )(
        new0,
        new1,
        rows_of(new2).reshape(TILES, 128),
        rows_of(update).reshape(TILES, 128),
        back.reshape(2 * N_DP * BACK, 128),
        back_rows,
    )
    master = new[2].reshape(RD // 8, COLS // 128, 8, 128).transpose(0, 2, 1, 3).reshape(RD, COLS)
    return (master, new[0].reshape(RD, COLS), new[1].reshape(RD, COLS))


def solution(mesh):
    specs = (P("dp", "tensor"),) * 4 + (P("dp", None),) * 2
    return jax.shard_map(
        per_device, mesh=mesh, in_specs=specs, out_specs=(P("dp", "tensor"),) * 3, check_vma=False
    )
```

```python
import functools

import jax
import jax.numpy as jnp
from jax import lax
from jax.experimental import pallas as pl
from jax.experimental.pallas import tpu as pltpu
from jax.sharding import PartitionSpec as P

ROWS = 3072
FF = 36864
SEGW = 128
RD = 48
COLS = 9216
HALF = 4608
NSEG = 36
BLOCKS = 1728
N_DP = 64
PER_PEER = 27
TILES = 2 * BLOCKS
MESH = pl.DeviceIdType.MESH

beta_one = 0.9
beta_two = 0.95
correct_one = 0.6513215599
correct_two = 0.4012630608
adam_eps = 1e-08
learning_rate = 0.01
weight_decay = 0.1
clip_ratio = 0.75

CHUNK = 512
EARLY = 3
FRONT = 21
BACK = PER_PEER - FRONT


def kernel(
    send_hbm, place_hbm, first_hbm, second_hbm, master_hbm, grad_hbm,
    new0, new1, new2, update, back, back_rows,
    old0, old1, old2, send0, send1, send2, recv0, recv1, front,
    grad, shard_rows, line_rows, plane_rows, slots, inverses, send_ref, place_ref, inverse_smem, front_smem,
    load_sems, table_sems, send_sem, recv_sems, small_send, small_recv, entered,
):
    me = lax.axis_index("dp")
    shard = lax.axis_index("tensor")
    z, x, core = me // 8, (me // 2) % 4, me % 2
    parity = shard % 2
    partner = shard + 1 - 2 * parity
    olds, sends = (old0, old1, old2), (send0, send1, send2)

    def dp_at(dz, dx, dc):
        return (((z + dz) % 8) * 4 + (x + dx) % 4) * 2 + (core + dc) % 2

    def signal(semaphore, j, t):
        pl.semaphore_signal(semaphore, inc=1, device_id=(j, t), device_id_type=MESH)

    barrier = pltpu.get_barrier_semaphore()
    for k in (4, 3, 5, 2, 6, 1, 7):
        signal(barrier, dp_at(k, 0, 0), shard)
    for k in (2, 1, 3):
        signal(barrier, dp_at(0, k, 0), shard)
    signal(barrier, dp_at(0, 0, 1), shard)
    for k in (1, 2, 3):
        signal(barrier, me, (shard + k) % 4)

    loads = [
        pltpu.make_async_copy(source, target, load_sems.at[k])
        for k, (source, target) in enumerate(
            [
                (send_hbm, send_ref),
                (first_hbm, old0),
                (second_hbm, old1),
                (master_hbm, old2),
                (grad_hbm, grad),
                (place_hbm, place_ref),
                (place_hbm, slots),
            ]
        )
    ]
    for load in loads[:2]:
        load.start()

    def offset_of(n):
        zi = n & 7
        dz = jnp.where((zi & 1) == 0, 4 + (zi >> 1), 3 - (zi >> 1))
        return (((z + dz) & 7) << 3) + (((x + (n >> 3)) & 3) << 1) + ((core + (n >> 5)) & 1)

    def gather(a, n):
        base = offset_of(n) * PER_PEER
        rows = [row_of(send_ref[0, base + q]) for q in range(PER_PEER)]
        for half in range(2):
            tiles = [olds[a][row + half * (NSEG * 8)] for row in rows]
            for q, tile in enumerate(tiles):
                sends[a][half * BLOCKS + base + q] = tile

    def deliver(a, j, t, half, target, first=0, count=PER_PEER):
        pltpu.make_async_remote_copy(
            src_ref=sends[min(a, 2)].at[pl.ds(half * BLOCKS + j * PER_PEER + first, count)],
            dst_ref=target.at[pl.ds((parity * N_DP + me) * count, count)],
            send_sem=send_sem,
            recv_sem=recv_sems.at[a],
            device_id=(j, t),
            device_id_type=MESH,
        ).start()

    def deliver_here(a, n):
        deliver(a, offset_of(n), shard, parity, recv0)

    def deliver_partner(a, n):
        deliver(a, offset_of(n), partner, 1 - parity, recv0)

    def gather_and_deliver(first, last):
        @pl.loop(first, last)
        def _(n):
            gather(0, n)
            deliver_here(0, n - 1)

    loads[0].wait()
    loads[1].wait()
    for load in loads[2:]:
        load.start()

    @pl.loop(0, EARLY)
    def _(n):
        gather(0, n)

    pl.semaphore_wait(barrier, 14)
    for k in (2, 1, 3):
        signal(entered.at[0], dp_at(0, k, 0), shard)

    @pl.loop(0, EARLY - 1)
    def _(n):
        deliver_here(0, n)

    gather_and_deliver(EARLY, 8)
    gather(0, 8)
    pl.semaphore_wait(entered.at[0], 3)
    signal(entered.at[1], dp_at(0, 0, 1), shard)
    gather_and_deliver(9, 33)
    pl.semaphore_wait(entered.at[1], 1)
    signal(entered.at[2], me, partner)
    gather_and_deliver(33, 64)
    pl.semaphore_wait(entered.at[2], 1)

    @pl.loop(0, 64)
    def _(n):
        deliver_partner(0, n)

    deliver_here(0, 63)

    loads[4].wait()

    def square(n, total):
        group = jnp.where(n >= 18, 1, 0) + jnp.where(n >= 36, 1, 0)
        columns = pl.ds(pl.multiple_of((n - 18 * group) * CHUNK, CHUNK), CHUNK)
        block = grad[group, :, columns].astype(jnp.float32)
        return total + block * block

    squares = lax.fori_loop(0, 54, square, jnp.zeros((16, CHUNK), jnp.float32))
    squares = jnp.sum(squares, axis=0, keepdims=True)
    shard_rows[shard] = squares[:, 0:128] + squares[:, 128:256] + squares[:, 256:384] + squares[:, 384:512]

    def pass_row(k, rows, own, j, t):
        pltpu.make_async_remote_copy(
            src_ref=rows.at[own],
            dst_ref=rows.at[own],
            send_sem=small_send.at[k],
            recv_sem=small_recv.at[k],
            device_id=(j, t),
            device_id_type=MESH,
        ).start()

    def wait_rows(rows, semaphore):
        others = rows.at[pl.ds(0, rows.shape[0] - 1)]
        pltpu.make_async_copy(others, others, semaphore).wait()

    def sum_of(rows):
        total = rows[0]
        for k in range(1, rows.shape[0]):
            total = total + rows[k]
        return total

    def gather_all(a):
        @pl.loop(0, 64)
        def _(n):
            gather(a, n)

    def deliver_all(a, *place):
        def peer(n):
            zi, xi = n & 7, (n >> 3) & 3
            dz = jnp.where((zi & 1) == 0, 4 + (zi >> 1), 3 - (zi >> 1))
            dx = jnp.where(xi == 0, 2, jnp.where(xi == 3, 0, 2 * xi - 1))
            return (((z + dz) & 7) << 3) + (((x + dx) & 3) << 1) + ((core + 1 - (n >> 5)) & 1)

        @pl.loop(0, 63)
        def _(n):
            deliver(a, peer(n), shard, parity, *place)
            deliver(a, peer(n), partner, 1 - parity, *place)

        deliver(a, me, partner, 1 - parity, *place)

    def keep(send, target, first=0, count=PER_PEER):
        target[pl.ds((parity * N_DP + me) * count, count)] = send[
            pl.ds(parity * BLOCKS + me * PER_PEER + first, count)
        ]

    keep(send0, recv0)
    loads[2].wait()
    gather_all(1)
    keep(send1, recv1)
    for k in (1, 2, 3):
        pass_row(0, shard_rows, shard, me, (shard + k) % 4)
    loads[3].wait()
    gather_all(2)
    keep(send2, front, 0, FRONT)
    keep(send2, back, FRONT, BACK)
    wait_rows(shard_rows, small_recv.at[0])
    line_rows[z * 2 + core] = sum_of(shard_rows)

    loads[5].wait()
    line = lax.broadcasted_iota(jnp.int32, (16, 128), 0)
    lane = lax.broadcasted_iota(jnp.int32, (16, 128), 1)
    group = jnp.where(line >= 5, 1, 0) + jnp.where(line >= 10, 1, 0)
    segment = (line - 5 * group) * 8 + (lane >> 4)
    ids = jnp.where((segment < NSEG) & (line < 15), (group * 16 + (lane & 15)) * NSEG + segment, -1)

    def find(i, tables):
        whole, part = tables
        for q in range(PER_PEER):
            k = i * PER_PEER + q
            here = ids == place_ref[0, k]
            whole = jnp.where(here, k, whole)
            if q < FRONT:
                part = jnp.where(here, i * FRONT + q, part)
        return whole, part

    zeros = jnp.zeros((16, 128), jnp.int32)
    whole, part = lax.fori_loop(0, N_DP, find, (zeros, zeros))
    inverses[0] = whole
    inverses[1] = part
    loads[6].wait()
    back_rows[...] = row_of(slots[...])
    table_copies = [
        pltpu.make_async_copy(inverses.at[0], inverse_smem, table_sems.at[0]),
        pltpu.make_async_copy(inverses.at[1], front_smem, table_sems.at[1]),
    ]
    for copy in table_copies:
        copy.start()

    for k in range(1, 16):
        pass_row(1, line_rows, z * 2 + core, dp_at(k >> 1, 0, k & 1), shard)
    deliver_all(1, recv1)
    for copy in table_copies:
        copy.wait()

    def arrive(a, recv, table, new):
        span = recv.at[pl.ds(0, recv.shape[0] * 127 // 128)]
        pltpu.make_async_copy(span, span, recv_sems.at[a]).wait()

        @pl.loop(0, 12)
        def _(n):
            place(recv, table, new, (n >> 2) * 5 + (n & 3), n >> 2, (n & 3) * 8, 8)

        @pl.loop(0, 3)
        def _(n):
            place(recv, table, new, n * 5 + 4, n, 32, 4)

    def each_chunk(body):
        @pl.loop(0, 54)
        def _(n):
            group = jnp.where(n >= 18, 1, 0) + jnp.where(n >= 36, 1, 0)
            body(group, pl.ds(pl.multiple_of((n - 18 * group) * CHUNK, CHUNK), CHUNK))

    wait_rows(line_rows, small_recv.at[1])
    plane_rows[x] = sum_of(line_rows)
    arrive(0, recv0, inverse_smem, new0)
    for k in (1, 2, 3):
        pass_row(2, plane_rows, x, dp_at(0, k, 0), shard)
    deliver_all(2, front, 0, FRONT)
    deliver_all(3, back, FRONT, BACK)
    arrive(1, recv1, inverse_smem, new1)

    wait_rows(plane_rows, small_recv.at[2])
    total = sum_of(plane_rows)
    sum_squares = jnp.sum(total, axis=(0, 1), keepdims=True)
    limit = clip_ratio * jnp.sqrt(jnp.float32(ROWS * FF))
    clip_scale = jnp.minimum(1.0, limit / jnp.sqrt(sum_squares + 1e-06))

    def first_step(group, columns):
        scaled = clip_scale * grad[group, :, columns].astype(jnp.float32)
        new0[group, :, columns] = beta_one * new0[group, :, columns] + (1.0 - beta_one) * scaled

    def second_step(group, columns):
        scaled = clip_scale * grad[group, :, columns].astype(jnp.float32)
        moment2 = beta_two * new1[group, :, columns] + (1.0 - beta_two) * scaled * scaled
        new1[group, :, columns] = moment2
        moment1 = new0[group, :, columns]
        update[group, :, columns] = moment1 / correct_one / (jnp.sqrt(moment2 / correct_two) + adam_eps)

    each_chunk(first_step)
    each_chunk(second_step)
    arrive(2, front, front_smem, new2)
    for rows, semaphore in zip((shard_rows, line_rows, plane_rows), range(3), strict=True):
        wait_rows(rows, small_send.at[semaphore])
    for a in range(3):
        span = sends[a].at[pl.ds(0, 127 * PER_PEER)]
        pltpu.make_async_copy(span, span, send_sem).wait()
    span = back.at[pl.ds(0, 127 * BACK)]
    pltpu.make_async_copy(span, span, recv_sems.at[3]).wait()


def row_of(slot):
    row = (slot * 1821) >> 16
    return slot * 8 + (row >> 3) * (COLS // 128 * 8) - row * (NSEG * 8) + (row & 7)


def place(recv, inverse, new, line, group, segment, count):
    for u in range(count):
        tiles = []
        for r in range(16):
            source = inverse[line, u * 16 + r]
            tiles.append((recv[source], recv[source + recv.shape[0] // 2]))
        for half in range(2):
            column = pl.ds(pl.multiple_of((half * NSEG + segment + u) * 128, 128), 128)
            for r in range(16):
                new[group, pl.ds(r, 1), column] = tiles[r][half]


def finish(new0, new1, new2, update, back, back_rows, first_out, second_out, master_out, master, rows_smem, sems):
    table = pltpu.make_async_copy(back_rows, rows_smem, sems.at[5])
    table.start()
    copies = [
        pltpu.make_async_copy(new0, first_out, sems.at[0]),
        pltpu.make_async_copy(new1, second_out, sems.at[1]),
    ]
    for copy in copies:
        copy.start()

    @pl.loop(0, TILES // 128)
    def _(n):
        rows = pl.ds(pl.multiple_of(n * 128, 128), 128)
        master[rows, :] = new2[rows, :]

    table.wait()

    @pl.loop(0, N_DP // 4)
    def _(n):
        for u in range(4):
            i = n * 4 + u
            rows = [rows_smem[0, i * PER_PEER + FRONT + q] for q in range(BACK)]
            for half in range(2):
                tiles = [back[pl.ds((half * N_DP + i) * BACK + q, 1), :] for q in range(BACK)]
                for row, tile in zip(rows, tiles, strict=True):
                    master[pl.ds(row + half * (NSEG * 8), 1), :] = tile

    third = TILES // 3
    for group in range(3):

        @pl.loop(0, third // 128)
        def _(n):
            rows = pl.ds(pl.multiple_of(group * third + n * 128, 128), 128)
            value = master[rows, :]
            master[rows, :] = value - learning_rate * (update[rows, :] + weight_decay * value)

        span = pl.ds(group * third, third)
        copy = pltpu.make_async_copy(master.at[span], master_out.at[span], sems.at[2 + group])
        copy.start()
        copies.append(copy)
    for copy in copies:
        copy.wait()


def per_device(master_old, moment1_old, moment2_old, grad, send_slots, recv_slots):
    def rows_of(matrix):
        return matrix.reshape(RD // 8, 8, COLS // 128, 128).transpose(0, 2, 1, 3).reshape(TILES, 1, 128)

    hbm = pl.BlockSpec(memory_space=pl.ANY)
    tiles = pltpu.VMEM((TILES, 1, 128), jnp.float32)
    whole = pltpu.VMEM((3, 16, COLS), jnp.float32)
    vmem = pl.BlockSpec(memory_space=pltpu.VMEM)
    new0, new1, new2, update, back, back_rows = pl.pallas_call(
        kernel,
        out_shape=[whole] * 4
        + [pltpu.VMEM((2 * N_DP * BACK, 1, 128), jnp.float32), pltpu.VMEM((1, BLOCKS), jnp.int32)],
        in_specs=[hbm] * 6,
        out_specs=[vmem] * 6,
        scratch_shapes=[tiles] * 8
        + [
            pltpu.VMEM((2 * N_DP * FRONT, 1, 128), jnp.float32),
            pltpu.VMEM((3, 16, COLS), jnp.bfloat16),
            pltpu.VMEM((4, 1, 128), jnp.float32),
            pltpu.VMEM((16, 1, 128), jnp.float32),
            pltpu.VMEM((4, 1, 128), jnp.float32),
            pltpu.VMEM((1, BLOCKS), jnp.int32),
            pltpu.VMEM((2, 16, 128), jnp.int32),
            pltpu.SMEM((1, BLOCKS), jnp.int32),
            pltpu.SMEM((1, BLOCKS), jnp.int32),
            pltpu.SMEM((16, 128), jnp.int32),
            pltpu.SMEM((16, 128), jnp.int32),
            pltpu.SemaphoreType.DMA((7,)),
            pltpu.SemaphoreType.DMA((2,)),
            pltpu.SemaphoreType.DMA,
            pltpu.SemaphoreType.DMA((4,)),
            pltpu.SemaphoreType.DMA((3,)),
            pltpu.SemaphoreType.DMA((3,)),
            pltpu.SemaphoreType.REGULAR((3,)),
        ],
        compiler_params=pltpu.CompilerParams(
            collective_id=0, has_side_effects=True, vmem_limit_bytes=56 * 2**20
        ),
    )(send_slots, recv_slots, rows_of(moment1_old), rows_of(moment2_old), rows_of(master_old), grad.reshape(3, 16, COLS))
    new = pl.pallas_call(
        finish,
        out_shape=[jax.ShapeDtypeStruct((3, 16, COLS), jnp.float32)] * 2
        + [jax.ShapeDtypeStruct((TILES, 128), jnp.float32)],
        in_specs=[vmem] * 6,
        out_specs=[hbm] * 3,
        scratch_shapes=[
            pltpu.VMEM((TILES, 128), jnp.float32),
            pltpu.SMEM((1, BLOCKS), jnp.int32),
            pltpu.SemaphoreType.DMA((6,)),
        ],
        compiler_params=pltpu.CompilerParams(vmem_limit_bytes=16 * 2**20),
    )(
        new0,
        new1,
        rows_of(new2).reshape(TILES, 128),
        rows_of(update).reshape(TILES, 128),
        back.reshape(2 * N_DP * BACK, 128),
        back_rows,
    )
    master = new[2].reshape(RD // 8, COLS // 128, 8, 128).transpose(0, 2, 1, 3).reshape(RD, COLS)
    return (master, new[0].reshape(RD, COLS), new[1].reshape(RD, COLS))


def solution(mesh):
    specs = (P("dp", "tensor"),) * 4 + (P("dp", None),) * 2
    return jax.shard_map(
        per_device, mesh=mesh, in_specs=specs, out_specs=(P("dp", "tensor"),) * 3, check_vma=False
    )
```
